32 devices in a mesh: dp: 8 (over z, y), tensor: 4 (over x, core).
Axes of the slice: x: 2, y: 2, z: 4, core: 2. Of those that a mesh axis runs over, the one named last changes fastest.
Arguments:
- tokens: bfloat16 [8192, 2048], P(('dp', 'tensor')), may hold values from -6 to 6
- lengths: int32 [8], P('dp'), may hold values from 256 to 1024, as said below
- ln1_gain: float32 [2048], replicated, may hold values from 0.5 to 1.5
- ln1_bias: float32 [2048], replicated, may hold values from -3 to 3
- w_query: bfloat16 [2048, 2048], P(None, 'tensor'), may hold values from -0.125 to 0.125
- w_key: bfloat16 [2048, 2048], P(None, 'tensor'), may hold values from -0.125 to 0.125
- w_value: bfloat16 [2048, 4096], P(None, 'tensor'), may hold values from -0.125 to 0.125
- w_gate: bfloat16 [2048, 4096], P(None, 'tensor'), may hold values from -0.125 to 0.125
- w_out: bfloat16 [4096, 2048], P('tensor'), may hold values from -0.1875 to 0.1875
- ln2_gain: float32 [2048], replicated, may hold values from 0.5 to 1.5
- ln2_bias: float32 [2048], replicated, may hold values from -3 to 3
- mlp_gate: bfloat16 [2048, 4096], P(None, 'tensor'), may hold values from -0.125 to 0.125
- mlp_up: bfloat16 [2048, 4096], P(None, 'tensor'), may hold values from -0.125 to 0.125
- mlp_down: bfloat16 [4096, 2048], P('tensor'), may hold values from -0.1875 to 0.1875
- cotangent: bfloat16 [8192, 2048], P(('dp', 'tensor')), may hold values from -6 to 6
Outputs:
- mixed: bfloat16 [8192, 2048], P(('dp', 'tensor'))
- grad_tokens: float32 [8192, 2048], P(('dp', 'tensor'))
- grad_ln1_gain: float32 [2048], P(('dp', 'tensor'))
- grad_ln1_bias: float32 [2048], P(('dp', 'tensor'))
- grad_w_query: float32 [2048, 2048], P('dp', 'tensor')
- grad_w_key: float32 [2048, 2048], P('dp', 'tensor')
- grad_w_value: float32 [2048, 4096], P('dp', 'tensor')
- grad_w_gate: float32 [2048, 4096], P('dp', 'tensor')
- grad_w_out: float32 [4096, 2048], P('tensor', 'dp')
- grad_ln2_gain: float32 [2048], P(('dp', 'tensor'))
- grad_ln2_bias: float32 [2048], P(('dp', 'tensor'))
- grad_mlp_gate: float32 [2048, 4096], P('dp', 'tensor')
- grad_mlp_up: float32 [2048, 4096], P('dp', 'tensor')
- grad_mlp_down: float32 [4096, 2048], P('tensor', 'dp')
The draws below stay inside these ranges and needn't reach their ends.
Inputs may be any that keep to these rules, and one draw needn't show every extreme that they name: Slot s holds one sequence in its first lengths[s] positions, the rest is padding; in every draw some slot is full (1024 tokens).
All inputs are finite; a program needn't handle non-finite values.
Results may differ from the reference program's by a relative error of at most 0.028.
Values may be sent and summed in bfloat16 or wider, within the bound.
A program may use at most 256 MiB of HBM per device.

```python
import jax
import jax.numpy as jnp
from jax import lax

D = 2048
HEADS = 8
KEY_HEAD = 256
VAL_HEAD = 512
FF = 4096
SEQ = 1024
SEQS_DP = 1
QK = 2048
VALS = 4096
SLOTS = 8
ROWS = 8192
N_DP = 8


def draw_lengths(key, part):
    first_key = jax.random.fold_in(key, 11)
    second_key = jax.random.fold_in(key, 23)
    drawn = jax.random.randint(first_key, (SLOTS,), SEQ // 4, SEQ + 1)
    full_slot = jax.random.randint(second_key, (), 0, SLOTS)
    return jnp.where(jnp.arange(SLOTS) == full_slot, SEQ, drawn).astype(jnp.int32)


def levels(stream_key, extent, pieces, smallest, high):
    gain, own = 1.0, jax.random.fold_in(stream_key, 6)
    for axis_at, blocks in pieces:
        steps = jnp.exp(jax.random.uniform(jax.random.fold_in(own, axis_at), (blocks,), jnp.float32, smallest / len(pieces), high / len(pieces)))
        gain = gain * jnp.repeat(steps, extent[axis_at] // blocks).reshape([-1 if axis == axis_at else 1 for axis in range(len(extent))])
    return gain


def gaussian(rng, extent, scale, reach, pieces=(), held_as=jnp.bfloat16):
    factor_of = levels(rng, extent, pieces, -0.22, 0.18) if pieces else 1.0
    values = jax.random.normal(rng, extent, jnp.float32) * scale * factor_of
    return jnp.minimum(jnp.maximum(values, -reach), reach).astype(held_as)


def setup_inputs(seed: int = 0) -> dict:
    splits = jax.random.split(jax.random.key(seed), 16)
    return {
        "tokens": gaussian(splits[0], (ROWS, D), 1.0, 6.0, ((0, 32),)),
        "lengths": draw_lengths(jax.random.fold_in(splits[15], 71), 0),
        "ln1_gain": jnp.clip(1.0 + 0.1 * jax.random.normal(splits[2], (D,), jnp.float32), 0.5, 1.5),
        "ln1_bias": gaussian(splits[3], (D,), 0.5, 3.0, (), jnp.float32),
        "w_query": gaussian(splits[4], (D, QK), D ** -0.5, 0.125, ((1, 4),)),
        "w_key": gaussian(splits[5], (D, QK), D ** -0.5, 0.125, ((1, 4),)),
        "w_value": gaussian(splits[6], (D, VALS), D ** -0.5, 0.125, ((1, 4),)),
        "w_gate": gaussian(splits[7], (D, VALS), D ** -0.5, 0.125, ((1, 4),)),
        "w_out": gaussian(splits[8], (VALS, D), (VALS // 4) ** -0.5, 0.1875, ((0, 4),)),
        "ln2_gain": jnp.clip(1.0 + 0.1 * jax.random.normal(splits[9], (D,), jnp.float32), 0.5, 1.5),
        "ln2_bias": gaussian(splits[10], (D,), 0.5, 3.0, (), jnp.float32),
        "mlp_gate": gaussian(splits[11], (D, FF), D ** -0.5, 0.125, ((1, 4),)),
        "mlp_up": gaussian(splits[12], (D, FF), D ** -0.5, 0.125, ((1, 4),)),
        "mlp_down": gaussian(splits[13], (FF, D), (FF // 4) ** -0.5, 0.1875, ((0, 4),)),
        "cotangent": gaussian(splits[14], (ROWS, D), 1.0, 6.0, ((0, 32),)),
    }


epsilon = 1e-05
highest = lax.Precision.HIGHEST

@jax.custom_vjp
def low(v):
    return lax.optimization_barrier(v.astype(jnp.bfloat16)).astype(jnp.float32)

@jax.custom_vjp
def low_back(v):
    return v

def low_keep(v):
    return (low(v), None)

def low_pass(kept, grad):
    return (grad,)

def back_keep(v):
    return (v, None)

def back_low(kept, grad):
    return (low(grad),)
low.defvjp(low_keep, low_pass)
low_back.defvjp(back_keep, back_low)

def product(left, right):
    return jnp.dot(left, right, precision=highest, preferred_element_type=jnp.float32)

def norm_rows(values, gain_in, bias_in):
    centre = values - lax.optimization_barrier(jnp.mean(values, axis=-1, keepdims=True))
    spread = lax.optimization_barrier(jnp.mean(centre * centre, axis=-1, keepdims=True))
    return centre * lax.rsqrt(spread + epsilon) * gain_in + bias_in

def rotate_pairs(values, angles):
    row_count, head_count, pair_width = values.shape
    paired = values.reshape(row_count, head_count, pair_width // 2, 2)
    first_part = paired[..., 0]
    second_part = paired[..., 1]
    cosine = jnp.cos(angles)[:, None, :]
    sine_part = jnp.sin(angles)[:, None, :]
    turned = jnp.stack((first_part * cosine - second_part * sine_part, second_part * cosine + first_part * sine_part), axis=-1)
    return turned.reshape(row_count, head_count, pair_width)

def retention(query_in, key_in, value_in, gate_in):
    row_count = query_in.shape[0]
    slot_count = row_count // SEQ
    position = (jnp.arange(row_count) % SEQ).astype(jnp.float32)
    angle_rate = 1.0 / 10000.0 ** jnp.linspace(0.0, 1.0, KEY_HEAD // 2)
    angles = position[:, None] * angle_rate[None, :]
    turned_query = rotate_pairs(query_in.reshape(row_count, HEADS, KEY_HEAD), angles).reshape(slot_count, SEQ, HEADS, KEY_HEAD)
    turned_key = (rotate_pairs(key_in.reshape(row_count, HEADS, KEY_HEAD), angles) * KEY_HEAD ** (-0.5)).reshape(slot_count, SEQ, HEADS, KEY_HEAD)
    values_all = value_in.reshape(slot_count, SEQ, HEADS, VAL_HEAD)
    log_decay = jnp.log(1.0 - 2.0 ** (-5.0 - jnp.arange(HEADS).astype(jnp.float32)))
    inner_index = jnp.arange(SEQ).astype(jnp.float32)
    offset_grid = inner_index[:, None] - inner_index[None, :]
    decay_grid = jnp.where(offset_grid[None] >= 0, jnp.exp(jnp.maximum(offset_grid, 0.0)[None] * log_decay[:, None, None]), 0.0)
    scores = jnp.einsum('snhd,smhd->shnm', turned_query, turned_key, precision=highest) * decay_grid[None]
    mixed_heads = jnp.einsum('shnm,smhe->snhe', scores, values_all, precision=highest).reshape(row_count, HEADS, VAL_HEAD)
    centre = mixed_heads - lax.optimization_barrier(jnp.mean(mixed_heads, axis=-1, keepdims=True))
    normed = centre * lax.rsqrt(jnp.maximum(lax.optimization_barrier(jnp.mean(centre * centre, axis=-1, keepdims=True)), 1.0))
    return jax.nn.silu(gate_in) * normed.reshape(row_count, HEADS * VAL_HEAD)

def block_layer(rows_in, weight_set):
    gain_one, bias_one, w_query, w_key, w_value, w_gate, w_out, gain_two, bias_two, mlp_gate, mlp_up, mlp_down = weight_set
    normed_one = low(norm_rows(rows_in, gain_one, bias_one))
    query_proj = low(low_back(product(normed_one, w_query)))
    key_proj = low(low_back(product(normed_one, w_key)))
    value_proj = low(low_back(product(normed_one, w_value)))
    gate_proj = low(low_back(product(normed_one, w_gate)))
    gated_out = low(retention(query_proj, key_proj, value_proj, gate_proj))
    branch_one = low_back(product(gated_out, w_out))
    middle = rows_in + branch_one
    normed_two = low(norm_rows(middle, gain_two, bias_two))
    gate_hidden = low_back(product(normed_two, mlp_gate))
    up_hidden = low_back(product(normed_two, mlp_up))
    hidden = low(jax.nn.gelu(gate_hidden, approximate=False) * up_hidden)
    branch_two = low_back(product(hidden, mlp_down))
    return middle + branch_two

def reference(tokens, lengths, ln1_gain, ln1_bias, w_query, w_key, w_value, w_gate, w_out, ln2_gain, ln2_bias, mlp_gate, mlp_up, mlp_down, cotangent):
    weight_set = tuple((weight.astype(jnp.float32) for weight in (ln1_gain, ln1_bias, w_query, w_key, w_value, w_gate, w_out, ln2_gain, ln2_bias, mlp_gate, mlp_up, mlp_down)))
    group_rows = SEQS_DP * SEQ
    stacked = tokens.astype(jnp.float32).reshape(N_DP, group_rows, D)
    kept_layer = jax.checkpoint(block_layer)

    def whole_layer(rows_all, weights_in):

        def one_group(carry, rows_in):
            return (carry, kept_layer(rows_in, weights_in))
        _, outputs = lax.scan(one_group, jnp.zeros((), jnp.float32), rows_all)
        return outputs
    result, pullback = jax.vjp(whole_layer, stacked, weight_set)
    valid_rows = (jnp.arange(SEQ)[None, :] < lengths[:, None]).astype(jnp.float32).reshape(N_DP, group_rows, 1)
    grad_rows, grad_weights = pullback(cotangent.astype(jnp.float32).reshape(N_DP, group_rows, D) * valid_rows)
    return (result.reshape(ROWS, D).astype(jnp.bfloat16), grad_rows.reshape(ROWS, D), grad_weights[0], grad_weights[1], grad_weights[2], grad_weights[3], grad_weights[4], grad_weights[5], grad_weights[6], grad_weights[7], grad_weights[8], grad_weights[9], grad_weights[10], grad_weights[11])
```

```python
import functools

import jax
import jax.numpy as jnp
from jax import lax
from jax.experimental import pallas as pl
from jax.experimental.pallas import tpu as pltpu
from jax.sharding import PartitionSpec as P

KEY_HEAD = 256
VAL_HEAD = 512
epsilon = 1e-05
BLOCK = 256
f32 = jnp.float32
bf16 = jnp.bfloat16


def swap_pairs(x):
    lane = lax.broadcasted_iota(jnp.int32, x.shape, 1)
    width = x.shape[1]
    return jnp.where(lane % 2 == 0, pltpu.roll(x, width - 1, 1), pltpu.roll(x, 1, 1))


def dot_nn(a, b):
    return lax.dot_general(a, b, (((1,), (0,)), ((), ())), preferred_element_type=f32)


def dot_nt(a, b):
    return lax.dot_general(a, b, (((1,), (1,)), ((), ())), preferred_element_type=f32)


def dot_tn(a, b):
    return lax.dot_general(a, b, (((0,), (0,)), ((), ())), preferred_element_type=f32)


def decay_blocks(log_decay, count):
    row = lax.broadcasted_iota(jnp.int32, (BLOCK, BLOCK), 0)
    col = lax.broadcasted_iota(jnp.int32, (BLOCK, BLOCK), 1)
    offset = (row - col).astype(f32)
    grids = [jnp.where(row >= col, jnp.exp(jnp.maximum(offset, 0.0) * log_decay), 0.0)]
    for d in range(1, count):
        grids.append(jnp.exp((offset + float(BLOCK * d)) * log_decay))
    return grids


def retain_kernel(
    rank_ref, decay_ref, qa, qb, ka, kb, va, vb, ga, gb, cos_ref, sin_ref,
    gated_ref, tq_ref, tk_ref, vc_ref, y_ref, stat_ref, wide_ref, grid_ref,
):
    rank = rank_ref[0]
    log_decay = decay_ref[pl.program_id(0)]
    blocks = gated_ref.shape[0] // BLOCK
    half = blocks // 2

    def part(first, second, s):
        ref = first if s < half else second
        return ref[(s % half) * BLOCK : (s % half + 1) * BLOCK, :]

    def rows_of(s):
        return pl.ds(pl.multiple_of((rank ^ s) * BLOCK, BLOCK), BLOCK)

    for s in range(blocks):
        rows = rows_of(s)
        cosine, sine = cos_ref[rows, :], sin_ref[rows, :]
        q = part(qa, qb, s).astype(f32)
        tq_ref[rows, :] = (q * cosine + swap_pairs(q) * sine).astype(bf16)
        k = part(ka, kb, s).astype(f32)
        tk_ref[rows, :] = (
            (k * cosine + swap_pairs(k) * sine) * KEY_HEAD ** (-0.5)
        ).astype(bf16)
        vc_ref[rows, :] = part(va, vb, s)
    for d, grid in enumerate(decay_blocks(log_decay, blocks)):
        grid_ref[d] = grid
    for i in range(blocks):
        lo = i * BLOCK
        q = tq_ref[lo : lo + BLOCK, :]
        total = jnp.zeros((BLOCK, VAL_HEAD), f32)
        for j in range(i + 1):
            k = tk_ref[j * BLOCK : (j + 1) * BLOCK, :]
            scores = (dot_nt(q, k) * grid_ref[i - j]).astype(bf16)
            total = total + dot_nn(scores, vc_ref[j * BLOCK : (j + 1) * BLOCK, :])
        centre = total - jnp.mean(total, axis=1, keepdims=True)
        var = jnp.mean(centre * centre, axis=1, keepdims=True)
        inverse = lax.rsqrt(jnp.maximum(var, 1.0))
        normed = centre * inverse
        wide_ref[lo : lo + BLOCK, :] = normed
        y_ref[lo : lo + BLOCK, :] = normed.astype(bf16)
        stat = jnp.where(var > 1.0, inverse, -inverse)
        stat_ref[lo : lo + BLOCK, :] = jnp.broadcast_to(stat, (BLOCK, 128))
    for s in range(blocks):
        gate = part(ga, gb, s).astype(f32)
        silu = gate / (1.0 + jnp.exp(-gate))
        gated_ref[s * BLOCK : (s + 1) * BLOCK, :] = (silu * wide_ref[rows_of(s), :]).astype(bf16)


def retain_back_kernel(
    rank_ref, decay_ref, gg_ref, tq_ref, tk_ref, vc_ref, y_ref, stat_ref, ga, gb, cos_ref, sin_ref,
    dq_ref, dk_ref, dv_ref, dg_ref, grad_ref, dq_wide, grid_ref,
):
    rank = rank_ref[0]
    log_decay = decay_ref[pl.program_id(0)]
    blocks = dq_ref.shape[0] // BLOCK
    half = blocks // 2

    def rows_of(s):
        return pl.ds(pl.multiple_of((rank ^ s) * BLOCK, BLOCK), BLOCK)

    for s in range(blocks):
        own = slice(s * BLOCK, (s + 1) * BLOCK)
        ref = ga if s < half else gb
        gate = ref[(s % half) * BLOCK : (s % half + 1) * BLOCK, :].astype(f32)
        grad = gg_ref[own, :].astype(f32)
        rows = rows_of(s)
        y = y_ref[rows, :].astype(f32)
        stat = stat_ref[rows, 0:1]
        sig = 1.0 / (1.0 + jnp.exp(-gate))
        silu = gate * sig
        dg_ref[own, :] = (grad * y * (sig * (1.0 + gate * (1.0 - sig)))).astype(bf16)
        e = grad * silu
        mean_e = jnp.mean(e, axis=1, keepdims=True)
        mean_ey = jnp.mean(e * y, axis=1, keepdims=True)
        pull = jnp.where(stat > 0.0, mean_ey, 0.0)
        grad_ref[rows, :] = ((e - mean_e - y * pull) * jnp.abs(stat)).astype(bf16)
    for d, grid in enumerate(decay_blocks(log_decay, blocks)):
        grid_ref[d] = grid

    def turn_back(x, rows):
        return x * cos_ref[rows, :] - swap_pairs(x) * sin_ref[rows, :]

    for j in range(blocks):
        cols = slice(j * BLOCK, (j + 1) * BLOCK)
        k = tk_ref[cols, :]
        v = vc_ref[cols, :]
        dv = jnp.zeros((BLOCK, VAL_HEAD), f32)
        dk = jnp.zeros((BLOCK, KEY_HEAD), f32)
        for i in range(j, blocks):
            rows = slice(i * BLOCK, (i + 1) * BLOCK)
            q = tq_ref[rows, :]
            g = grad_ref[rows, :]
            decay = grid_ref[i - j]
            scores = (dot_nt(q, k) * decay).astype(bf16)
            pulled = (dot_nt(g, v) * decay).astype(bf16)
            dv = dv + dot_tn(scores, g)
            dk = dk + dot_tn(pulled, q)
            dq = dot_nn(pulled, k)
            if j == 0:
                dq_wide[rows, :] = dq
            else:
                dq_wide[rows, :] = dq_wide[rows, :] + dq
        out = pl.ds(pl.multiple_of((rank ^ j) * BLOCK, BLOCK), BLOCK)
        dv_ref[out, :] = dv.astype(bf16)
        dk_ref[out, :] = (turn_back(dk, cols) * KEY_HEAD ** (-0.5)).astype(bf16)
        dq_ref[out, :] = turn_back(dq_wide[cols, :], cols).astype(bf16)


def retain(rank, decay, q, k, v, g, cosine, sine):
    rows = 2 * q[0].shape[0]
    half = rows // 2
    heads = q[0].shape[1] // KEY_HEAD
    smem = pl.BlockSpec(memory_space=pltpu.SMEM)
    narrow = pl.BlockSpec((half, KEY_HEAD), lambda h: (0, h))
    wide = pl.BlockSpec((half, VAL_HEAD), lambda h: (0, h))
    table = pl.BlockSpec((rows, KEY_HEAD), lambda h: (0, 0), pipeline_mode=pl.Buffered(1))
    out_n = pl.BlockSpec((rows, KEY_HEAD), lambda h: (0, h))
    out_w = pl.BlockSpec((rows, VAL_HEAD), lambda h: (0, h))
    stat = pl.BlockSpec((rows, 128), lambda h: (0, h))
    shape = jax.ShapeDtypeStruct
    return pl.pallas_call(
        retain_kernel,
        grid=(heads,),
        in_specs=[smem, smem, narrow, narrow, narrow, narrow, wide, wide, wide, wide, table, table],
        out_specs=[out_w, out_n, out_n, out_w, out_w, stat],
        out_shape=[
            shape((rows, heads * VAL_HEAD), bf16),
            shape((rows, heads * KEY_HEAD), bf16),
            shape((rows, heads * KEY_HEAD), bf16),
            shape((rows, heads * VAL_HEAD), bf16),
            shape((rows, heads * VAL_HEAD), bf16),
            shape((rows, heads * 128), f32),
        ],
        scratch_shapes=[
            pltpu.VMEM((rows, VAL_HEAD), f32),
            pltpu.VMEM((rows // BLOCK, BLOCK, BLOCK), f32),
        ],
        cost_estimate=pl.CostEstimate(
            flops=4_000_000_000, bytes_accessed=16_000_000, transcendentals=2_000_000
        ),
        name="retain_forward",
    )(rank, decay, *q, *k, *v, *g, cosine, sine)


def retain_back(rank, decay, grad_gated, tq, tk, vc, y, stat_in, g, cosine, sine):
    rows = grad_gated.shape[0]
    half = rows // 2
    heads = tq.shape[1] // KEY_HEAD
    smem = pl.BlockSpec(memory_space=pltpu.SMEM)
    wide = pl.BlockSpec((half, VAL_HEAD), lambda h: (0, h))
    table = pl.BlockSpec((rows, KEY_HEAD), lambda h: (0, 0), pipeline_mode=pl.Buffered(1))
    out_n = pl.BlockSpec((rows, KEY_HEAD), lambda h: (0, h))
    out_w = pl.BlockSpec((rows, VAL_HEAD), lambda h: (0, h))
    stat = pl.BlockSpec((rows, 128), lambda h: (0, h))
    shape = jax.ShapeDtypeStruct
    return pl.pallas_call(
        retain_back_kernel,
        grid=(heads,),
        in_specs=[smem, smem, out_w, out_n, out_n, out_w, out_w, stat, wide, wide, table, table],
        out_specs=[out_n, out_n, out_w, out_w],
        out_shape=[
            shape((rows, heads * KEY_HEAD), bf16),
            shape((rows, heads * KEY_HEAD), bf16),
            shape((rows, heads * VAL_HEAD), bf16),
            shape((rows, heads * VAL_HEAD), bf16),
        ],
        scratch_shapes=[
            pltpu.VMEM((rows, VAL_HEAD), bf16),
            pltpu.VMEM((rows, KEY_HEAD), f32),
            pltpu.VMEM((rows // BLOCK, BLOCK, BLOCK), f32),
        ],
        cost_estimate=pl.CostEstimate(
            flops=8_000_000_000, bytes_accessed=20_000_000, transcendentals=3_000_000
        ),
        name="retain_backward",
    )(rank, decay, grad_gated, tq, tk, vc, y, stat_in, *g, cosine, sine)


def gate_up_kernel(xa, xb, wg_ref, wu_ref, hidden_ref, gelu_ref, slope_ref, rows_ref):
    top = xa.shape[0]

    @pl.when(pl.program_id(0) == 0)
    def _():
        rows_ref[:top, :] = xa[...]
        rows_ref[top:, :] = xb[...]

    gate = dot_nn(rows_ref[...], wg_ref[...])
    up = dot_nn(rows_ref[...], wu_ref[...])
    phi = 0.5 * (1.0 + lax.erf(gate * 0.7071067811865476))
    gelu = gate * phi
    density = jnp.exp(-0.5 * gate * gate) * 0.3989422804014327
    hidden_ref[...] = (gelu * up).astype(bf16)
    gelu_ref[...] = gelu.astype(bf16)
    slope_ref[...] = (up * (phi + gate * density)).astype(bf16)


def gate_up(xa, xb, wg, wu):
    rows = xa.shape[0] + xb.shape[0]
    depth, cols = wg.shape
    wide = 256
    full = pl.BlockSpec(xa.shape, lambda n: (0, 0), pipeline_mode=pl.Buffered(1))
    weight = pl.BlockSpec((depth, wide), lambda n: (0, n))
    out = pl.BlockSpec((rows, wide), lambda n: (0, n))
    shape = jax.ShapeDtypeStruct((rows, cols), bf16)
    return pl.pallas_call(
        gate_up_kernel,
        grid=(cols // wide,),
        in_specs=[full, full, weight, weight],
        out_specs=[out, out, out],
        out_shape=[shape, shape, shape],
        scratch_shapes=[pltpu.VMEM((rows, depth), bf16)],
        cost_estimate=pl.CostEstimate(
            flops=4 * rows * depth * cols,
            bytes_accessed=2 * (rows * depth + 2 * depth * cols + 3 * rows * cols),
            transcendentals=2 * rows * cols,
        ),
        name="gate_up",
    )(xa, xb, wg, wu)


def mm(a, b):
    return jnp.dot(a, b, preferred_element_type=f32)


def contract_rows(left, right):
    return lax.dot_general(left, right, (((0,), (0,)), ((), ())), preferred_element_type=f32)


def contract_cols(left, right):
    return lax.dot_general(left, right, (((1,), (1,)), ((), ())), preferred_element_type=f32)


def norm_stats(values):
    mean = jnp.mean(values, axis=-1, keepdims=True)
    centre = values - mean
    spread = jnp.mean(centre * centre, axis=-1, keepdims=True)
    inverse = lax.rsqrt(spread + epsilon)
    return centre * inverse, inverse


def norm_back(hat, inverse, gain, grad):
    e = grad * gain
    pulled = (
        e - jnp.mean(e, axis=-1, keepdims=True) - hat * jnp.mean(e * hat, axis=-1, keepdims=True)
    ) * inverse
    return pulled, jnp.sum(grad * hat, axis=0), jnp.sum(grad, axis=0)


def make_local(n_dp, n_tensor):
    dp_bits = n_dp.bit_length() - 1

    def hop(value, axis, bit):
        size = n_dp if axis == "dp" else n_tensor
        return lax.ppermute(value, axis, [(i, i ^ bit) for i in range(size)])

    def spread(own):
        far = hop(own, "tensor", 2)
        near = hop(own, "tensor", 1)
        both = hop(far, "tensor", 1)
        return own, near, far, both

    def collect(part_of):
        rows = BLOCK
        from_both = hop(part_of(3).astype(bf16), "tensor", 1)
        far = (part_of(2) + from_both.astype(f32)).astype(bf16)
        from_far = hop(far, "tensor", 2)
        from_near = hop(part_of(1).astype(bf16), "tensor", 1)
        return part_of(0) + from_near.astype(f32) + from_far.astype(f32)

    def columns(values, rank, order):
        width = values.shape[1] // n_dp
        pieces = []
        for position in range(n_dp):
            block = 0
            for place, bit in enumerate(order):
                block |= ((position >> (len(order) - 1 - place)) & 1) << bit
            pieces.append(
                lax.dynamic_slice_in_dim(values, (rank ^ block) * width, width, axis=1)
            )
        middle = n_dp // 2
        return jnp.concatenate(pieces[:middle], axis=1), jnp.concatenate(pieces[middle:], axis=1)

    def halves(values, axis):
        size = values.shape[axis] // 2
        return (
            lax.slice_in_dim(values, 0, size, axis=axis),
            lax.slice_in_dim(values, size, 2 * size, axis=axis),
        )

    def reduce_dp(keep, send, order, axis):
        got = hop(send.astype(bf16), "dp", 1 << order[0])
        for bit in order[1:]:
            keep_a, keep_b = halves(keep, axis)
            got_a, got_b = halves(got, axis)
            send = (keep_b.astype(f32) + got_b.astype(f32)).astype(bf16)
            keep = (keep_a.astype(f32) + got_a.astype(f32)).astype(bf16)
            got = hop(send, "dp", 1 << bit)
        return keep.astype(f32) + got.astype(f32)

    def all_sum(value):
        for bit in range(n_tensor.bit_length() - 1):
            value = value + hop(value, "tensor", 1 << bit)
        for bit in range(dp_bits):
            value = value + hop(value, "dp", 1 << bit)
        return value

    def local(
        tokens, lengths, ln1_gain, ln1_bias, w_query, w_key, w_value, w_gate, w_out,
        ln2_gain, ln2_bias, mlp_gate, mlp_up, mlp_down, cotangent,
    ):
        own_rows = tokens.shape[0]
        seq = own_rows * n_tensor
        rank = lax.axis_index("tensor")
        dp_rank = lax.axis_index("dp")
        heads = w_query.shape[1] // KEY_HEAD
        order_a = tuple(range(dp_bits))
        order_b = (1, 0) + tuple(range(2, dp_bits))
        rank_in = rank.astype(jnp.int32)[None]
        head_ids = (rank * heads + jnp.arange(heads)).astype(f32)
        decay = jnp.log(1.0 - 2.0 ** (-5.0 - head_ids))

        tokens_wide = tokens.astype(f32)
        hat_one, inverse_one = norm_stats(tokens_wide)
        sent_one = (hat_one * ln1_gain + ln1_bias).astype(bf16)
        x0, x1, x2, x3 = spread(sent_one)

        position = jnp.arange(seq).astype(f32)
        angle_rate = jnp.repeat(1.0 / 10000.0 ** jnp.linspace(0.0, 1.0, KEY_HEAD // 2), 2)
        angles = position[:, None] * angle_rate[None, :]
        cosine = jnp.cos(angles)
        sign = jnp.where(jnp.arange(KEY_HEAD) % 2 == 0, -1.0, 1.0)
        sine = jnp.sin(angles) * sign[None, :]

        row_ids = rank * own_rows + jnp.arange(own_rows)
        valid = (row_ids < lengths[0]).astype(f32)
        out_grad = cotangent.astype(f32) * valid[:, None]
        out_low, _ = lax.optimization_barrier((out_grad.astype(bf16), x2))
        c0, c1, c2, c3 = spread(out_low)

        top = jnp.concatenate((x0, x1), axis=0)
        bottom = jnp.concatenate((x2, x3), axis=0)
        proj = [
            tuple(mm(part, w).astype(bf16) for part in (top, bottom))
            for w in (w_query, w_key, w_value, w_gate)
        ]
        gated, tq, tk, vc, y, stat = retain(rank_in, decay, *proj, cosine, sine)
        branch_one = collect(
            lambda s: mm(lax.slice_in_dim(gated, s * own_rows, (s + 1) * own_rows, axis=0), w_out)
        )
        middle = tokens_wide + branch_one
        hat_two, inverse_two = norm_stats(middle)
        sent_two = (hat_two * ln2_gain + ln2_bias).astype(bf16)
        z0, z1, z2, z3 = spread(sent_two)
        hid_a, gelu_a, slope_a = gate_up(z0, z1, mlp_gate, mlp_up)
        hid_b, gelu_b, slope_b = gate_up(z2, z3, mlp_gate, mlp_up)
        hidden = jnp.concatenate((hid_a, hid_b), axis=0)
        gelu = jnp.concatenate((gelu_a, gelu_b), axis=0)
        slope = jnp.concatenate((slope_a, slope_b), axis=0)

        grads = jnp.concatenate((c0, c1, c2, c3), axis=0)
        keep_x, send_x = columns(grads, dp_rank, order_a)
        grad_down = reduce_dp(
            contract_rows(hidden, keep_x), contract_rows(hidden, send_x), order_a, 1
        )
        grad_hidden = contract_cols(grads, mlp_down)
        grad_gate_hidden = (grad_hidden * slope.astype(f32)).astype(bf16)
        grad_up_hidden = (grad_hidden * gelu.astype(f32)).astype(bf16)

        rows_two = jnp.concatenate((z0, z1, z2, z3), axis=0)
        keep_x, send_x = columns(rows_two, dp_rank, order_a)
        grad_gate_weight = reduce_dp(
            contract_rows(keep_x, grad_gate_hidden), contract_rows(send_x, grad_gate_hidden), order_a, 0
        )
        grad_up_weight = reduce_dp(
            contract_rows(keep_x, grad_up_hidden), contract_rows(send_x, grad_up_hidden), order_a, 0
        )

        def take(values, s):
            return lax.slice_in_dim(values, s * own_rows, (s + 1) * own_rows, axis=0)

        branch_two = collect(lambda s: mm(take(hidden, s), mlp_down))
        mixed_out = (middle + branch_two).astype(bf16)

        grad_normed_two = collect(
            lambda s: contract_cols(take(grad_gate_hidden, s), mlp_gate)
            + contract_cols(take(grad_up_hidden, s), mlp_up)
        )
        pulled, grad_gain_two, grad_bias_two = norm_back(
            hat_two, inverse_two, ln2_gain, grad_normed_two
        )
        grad_middle = out_grad + pulled
        b0, b1, b2, b3 = spread(grad_middle.astype(bf16))
        grad_rows = jnp.concatenate((b0, b1, b2, b3), axis=0)
        keep_x, send_x = columns(grad_rows, dp_rank, order_a)
        grad_out_weight = reduce_dp(
            contract_rows(gated, keep_x), contract_rows(gated, send_x), order_a, 1
        )
        grad_gated = contract_cols(grad_rows, w_out).astype(bf16)
        dq, dk, dv, dg = retain_back(
            rank_in, decay, grad_gated, tq, tk, vc, y, stat, proj[3], cosine, sine
        )
        rows_one = jnp.concatenate((x0, x1, x2, x3), axis=0)
        keep_x, send_x = columns(rows_one, dp_rank, order_a)

        def weight_one(grad):
            return reduce_dp(
                contract_rows(keep_x, grad), contract_rows(send_x, grad), order_a, 0
            )

        grad_value_weight = weight_one(dv)
        grad_gate_weight_one = weight_one(dg)
        keep_x, send_x = columns(rows_one, dp_rank, order_b)

        def weight_two(grad):
            return reduce_dp(
                contract_rows(keep_x, grad), contract_rows(send_x, grad), order_b, 0
            )

        grad_query_weight = weight_two(dq)
        grad_key_weight = weight_two(dk)
        grad_normed_one = collect(
            lambda s: contract_cols(take(dq, s), w_query)
            + contract_cols(take(dk, s), w_key)
            + contract_cols(take(dv, s), w_value)
            + contract_cols(take(dg, s), w_gate)
        )
        pulled, grad_gain_one, grad_bias_one = norm_back(
            hat_one, inverse_one, ln1_gain, grad_normed_one
        )
        grad_tokens = grad_middle + pulled

        width = ln1_gain.shape[0] // (n_dp * n_tensor)
        start = (dp_rank * n_tensor + rank) * width

        def norm_term(*terms):
            summed = all_sum(jnp.stack(terms))
            return lax.dynamic_slice_in_dim(summed, start, width, axis=1)

        norm_two = norm_term(grad_gain_two, grad_bias_two)
        norm_one = norm_term(grad_gain_one, grad_bias_one)
        return (
            mixed_out,
            grad_tokens,
            norm_one[0],
            norm_one[1],
            grad_query_weight,
            grad_key_weight,
            grad_value_weight,
            grad_gate_weight_one,
            grad_out_weight,
            norm_two[0],
            norm_two[1],
            grad_gate_weight,
            grad_up_weight,
            grad_down,
        )

    return local


def solution(mesh):
    in_specs = (
        P(("dp", "tensor"), None),
        P("dp"),
        P(),
        P(),
        P(None, "tensor"),
        P(None, "tensor"),
        P(None, "tensor"),
        P(None, "tensor"),
        P("tensor", None),
        P(),
        P(),
        P(None, "tensor"),
        P(None, "tensor"),
        P("tensor", None),
        P(("dp", "tensor"), None),
    )
    out_specs = (
        P(("dp", "tensor"), None),
        P(("dp", "tensor"), None),
        P(("dp", "tensor")),
        P(("dp", "tensor")),
        P("dp", "tensor"),
        P("dp", "tensor"),
        P("dp", "tensor"),
        P("dp", "tensor"),
        P("tensor", "dp"),
        P(("dp", "tensor")),
        P(("dp", "tensor")),
        P("dp", "tensor"),
        P("dp", "tensor"),
        P("tensor", "dp"),
    )
    local = make_local(mesh.shape["dp"], mesh.shape["tensor"])
    return jax.shard_map(local, mesh=mesh, in_specs=in_specs, out_specs=out_specs, check_vma=False)
```
